32 devices in a mesh: view: 4 (over x, core), gz: 8 (over z, y).
Axes of the slice: x: 2, y: 2, z: 4, core: 2. Of those that a mesh axis runs over, the one named last changes fastest.
Arguments:
- views_data: float32 [4, 128, 128, 384], P('view', 'gz'), may hold values from 0.25 to 4
- start: float32 [128, 128, 384], P('gz'), may hold values from 0.5 to 2
- psf_table: float32 [8, 3, 17], replicated, may hold values from 0.05 to 1
- psf_index: int32 [4], P('view'), may hold values from 0 to 7
Outputs:
- estimate: float32 [128, 128, 384], P('gz')
The draws below stay inside these ranges and needn't reach their ends.
All inputs are finite; a program needn't handle non-finite values.
Results may differ from the reference program's by a relative error of at most 0.0001.
Values sent between devices are 32-bit elements; how exact they have to be, the bound alone decides.
A program may use at most 128 MiB of HBM per device.

```python
import math
import jax
import jax.numpy as jnp
from jax import lax

NX = 128
NY = 384
RAD = 8
ITERS = 2
NPSF = 8
VIEWS = 4
TAPS = 17
NZ = 128


def plant(result, rng, least, high):
    extent = result.shape
    place = [jax.random.randint(jax.random.fold_in(rng, axis), (), 0, extent[axis]) for axis in range(len(extent))]
    result = result.at[tuple(place)].set(least)
    longest = extent.index(max(extent))
    place[longest] = (place[longest] + 1) % extent[longest]
    return result.at[tuple(place)].set(high)


def level_of(stream_key, shape, shards, smallest, high):
    def one(position, shards_of):
        steps = jax.random.uniform(jax.random.fold_in(jax.random.fold_in(stream_key, 6), position), (shards_of,), jnp.float32, smallest / len(shards), high / len(shards))
        return jnp.repeat(jnp.exp(steps), shape[position] // shards_of).reshape((-1,) + (1,) * (len(shape) - position - 1))

    gain = one(*shards[0])
    for cut in shards[1:]:
        gain = gain * one(*cut)
    return gain


def setup_inputs(seed: int = 0) -> dict:
    arg_keys = jax.random.split(jax.random.key(seed), 5)
    return {
        "views_data": jnp.clip(jnp.exp(math.log(4.0) - 2.7725887 * jax.random.uniform(arg_keys[0], (VIEWS, NZ, NX, NY), jnp.float32) ** level_of(arg_keys[0], (VIEWS, NZ, NX, NY), ((0, 4), (1, 8)), -0.2, 0.2)), 0.25, 4.0),
        "start": jnp.clip(jnp.exp(math.log(2.0) - 1.3862944 * jax.random.uniform(arg_keys[1], (NZ, NX, NY), jnp.float32) ** level_of(arg_keys[1], (NZ, NX, NY), ((0, 8),), -0.2, 0.2)), 0.5, 2.0),
        "psf_table": jnp.clip(jnp.exp(jax.random.uniform(arg_keys[2], (NPSF, 3, TAPS), jnp.float32, math.log(0.05), math.log(1.0))), 0.05, 1.0),
        "psf_index": plant(jax.random.randint(arg_keys[3], (VIEWS,), 0, NPSF), jax.random.fold_in(arg_keys[3], 1), 0, NPSF - 1).astype(jnp.int32),
    }


def band_matrix(kern_row, length):
    places = jnp.arange(length)
    offsets = places[None, :] - places[:, None]
    tap_shift = jnp.arange(2 * RAD + 1) - RAD
    matches = (offsets[None, :, :] == tap_shift[:, None, None]).astype(jnp.float32)
    return jnp.sum(kern_row[:, None, None] * matches, axis=0)


def blur_planes(volume, mat_x, mat_y):
    along_x = jnp.einsum("ij,zjy->ziy", mat_x, volume, precision=lax.Precision.HIGHEST)
    return jnp.einsum("zxj,ij->zxi", along_x, mat_y, precision=lax.Precision.HIGHEST)


def back_planes(volume, mat_x, mat_y):
    along_x = jnp.einsum("ij,ziy->zjy", mat_x, volume, precision=lax.Precision.HIGHEST)
    return jnp.einsum("zxi,ij->zxj", along_x, mat_y, precision=lax.Precision.HIGHEST)


def forward_z(padded, kern_z, rows):
    total = kern_z[0] * padded[0:rows]
    for tap in range(1, 2 * RAD + 1):
        total = total + kern_z[tap] * padded[tap:tap + rows]
    return total


def backward_z(padded, kern_z, rows):
    total = kern_z[0] * padded[2 * RAD:2 * RAD + rows]
    for tap in range(1, 2 * RAD + 1):
        total = total + kern_z[tap] * padded[2 * RAD - tap:2 * RAD - tap + rows]
    return total


def reference(views_data, start, psf_table, psf_index):
    estimate = start
    widths = ((RAD, RAD), (0, 0), (0, 0))
    for step in range(ITERS):
        total = None
        for which in range(VIEWS):
            kern = psf_table[psf_index[which]]
            kern = kern / jnp.sum(kern, axis=-1, keepdims=True)
            mat_x = band_matrix(kern[1], NX)
            mat_y = band_matrix(kern[2], NY)
            planes = blur_planes(estimate, mat_x, mat_y)
            blurred = forward_z(jnp.pad(planes, widths), kern[0], NZ)
            ratio = views_data[which] / blurred
            smeared = backward_z(jnp.pad(ratio, widths), kern[0], NZ)
            correction = back_planes(smeared, mat_x, mat_y)
            total = correction if total is None else total * correction
        estimate = estimate * jnp.power(total, 1.0 / VIEWS)
    return estimate
```

```python
import functools
import jax
import jax.numpy as jnp
from jax import lax
from jax.experimental import pallas as pl
from jax.experimental.pallas import tpu as pltpu
from jax.sharding import PartitionSpec as P

ITERS = 2
AXES = ("view", "gz")
GROUP = 4
VMEM = pl.BlockSpec(memory_space=pltpu.VMEM)
SMEM = pl.BlockSpec(memory_space=pltpu.SMEM)
PARAMS = pltpu.CompilerParams(vmem_limit_bytes=40 * 1024 * 1024)


def split(value):
    high = value.astype(jnp.bfloat16)
    return high, (value - high.astype(jnp.float32)).astype(jnp.bfloat16)


def dot3(lhs, rhs):
    (lh, ll), (rh, rl) = lhs, rhs
    dot = functools.partial(jnp.dot, preferred_element_type=jnp.float32)
    return dot(lh, rh) + (dot(ll, rh) + dot(lh, rl))


def taps_sum(kz_ref, source, flip):
    taps = kz_ref.shape[0]
    total = kz_ref[taps - 1 if flip else 0] * source(0)
    for tap in range(1, taps):
        total = total + kz_ref[taps - 1 - tap if flip else tap] * source(tap)
    return total


def forward_kernel(kz_ref, e_ref, d_ref, ax_ref, my_ref, r_ref, zc_ref):
    rows_in, width = e_ref.shape[1], e_ref.shape[2]
    rows = d_ref.shape[1]
    ax = split(ax_ref[...])
    my = split(my_ref[...])

    @pl.loop(0, d_ref.shape[0] // GROUP)
    def _(step):
        base = step * GROUP
        for plane in range(GROUP):
            for tile in range(rows_in // 8):
                at = pl.ds(tile * 8, 8)
                zc_ref[pl.ds(plane * rows_in + tile * 8, 8), :] = taps_sum(
                    kz_ref, lambda tap: e_ref[base + plane + tap, at, :], False
                )
        along_x = dot3(ax, split(zc_ref[...]))
        blurred = dot3(split(along_x), my)
        r_ref[pl.ds(base, GROUP)] = d_ref[pl.ds(base, GROUP)] / blurred.reshape(GROUP, rows, width)


def smear_kernel(kz_ref, low_ref, r_ref, high_ref, u_ref):
    planes, pad = r_ref.shape[0], low_ref.shape[0]

    def source(place):
        if place < pad:
            return low_ref[place]
        if place < pad + planes:
            return r_ref[place - pad]
        return high_ref[place - pad - planes]

    for plane in range(planes):
        u_ref[plane] = taps_sum(kz_ref, lambda tap: source(plane + tap), True)


def back_kernel(low_ref, u_ref, high_ref, ax_ref, my_ref, *rest):
    out_ref, wide_ref = rest[-2:]
    rows, width = u_ref.shape[1], u_ref.shape[2]
    pad = low_ref.shape[1]
    wide = rows + 2 * pad
    ax = split(ax_ref[...])
    my = split(my_ref[...])

    @pl.loop(0, u_ref.shape[0] // GROUP)
    def _(step):
        base = step * GROUP
        for plane in range(GROUP):
            wide_ref[pl.ds(plane * wide, pad), :] = low_ref[base + plane]
            wide_ref[pl.ds(plane * wide + pad, rows), :] = u_ref[base + plane]
            wide_ref[pl.ds(plane * wide + pad + rows, pad), :] = high_ref[base + plane]
        along_x = dot3(ax, split(wide_ref[...]))
        result = dot3(split(along_x), my).reshape(GROUP, rows, width)
        if len(rest) == 3:
            result = result * rest[0][pl.ds(base, GROUP)]
        out_ref[pl.ds(base, GROUP)] = result


def blur_forward(kz, wide, data, ax, my):
    planes, rows, width = data.shape
    return pl.pallas_call(
        forward_kernel,
        out_shape=jax.ShapeDtypeStruct(data.shape, jnp.float32),
        in_specs=[SMEM, VMEM, VMEM, VMEM, VMEM],
        out_specs=VMEM,
        scratch_shapes=[pltpu.VMEM((GROUP * wide.shape[1], width), jnp.float32)],
        compiler_params=PARAMS,
        cost_estimate=pl.CostEstimate(
            flops=data.size * 2 * width * 12, bytes_accessed=16 * data.size, transcendentals=0
        ),
    )(kz, wide, data, ax, my)


def smear(kz, low, ratio, high):
    planes, rows, width = ratio.shape
    pad = low.shape[0]
    block = lambda depth: pl.BlockSpec((depth, 8, width), lambda i: (0, i, 0))
    return pl.pallas_call(
        smear_kernel,
        grid=(rows // 8,),
        out_shape=jax.ShapeDtypeStruct(ratio.shape, jnp.float32),
        in_specs=[SMEM, block(pad), block(planes), block(pad)],
        out_specs=block(planes),
        compiler_params=PARAMS,
        cost_estimate=pl.CostEstimate(
            flops=ratio.size * 2 * width * 6, bytes_accessed=12 * ratio.size, transcendentals=0
        ),
    )(kz, low, ratio, high)


def blur_back(low, u, high, ax, my, other):
    planes, rows, width = u.shape
    extra = [] if other is None else [other]
    return pl.pallas_call(
        back_kernel,
        out_shape=jax.ShapeDtypeStruct(u.shape, jnp.float32),
        in_specs=[VMEM] * (5 + len(extra)),
        out_specs=VMEM,
        scratch_shapes=[pltpu.VMEM((GROUP * (rows + 2 * low.shape[1]), width), jnp.float32)],
        compiler_params=PARAMS,
        cost_estimate=pl.CostEstimate(
            flops=u.size * 2 * width * 6, bytes_accessed=12 * u.size, transcendentals=0
        ),
    )(low, u, high, ax, my, *extra)


def banded(kern_row, outputs, inputs, shift):
    tap = jnp.arange(inputs)[None, :] - jnp.arange(outputs)[:, None] + shift
    taps = jnp.arange(kern_row.shape[0])
    return jnp.sum(jnp.where(tap[None] == taps[:, None, None], kern_row[:, None, None], 0.0), axis=0)


def x_matrix(kern_row, rows, pad):
    one = banded(kern_row, rows, rows + 2 * pad, 0)
    eye = jnp.eye(GROUP, dtype=jnp.float32)
    return (eye[:, None, :, None] * one[None, :, None, :]).reshape(
        GROUP * rows, GROUP * (rows + 2 * pad)
    )


def on_device(sections, count, views_data, start, psf_table, psf_index):
    slab = views_data[0]
    planes, width_x, width_y = start.shape
    pad = (psf_table.shape[2] - 1) // 2
    share = width_x // 4
    half = planes // 2
    view, gz = lax.axis_index("view"), lax.axis_index("gz")
    a, c, b = view // 2, view % 2, gz % 2

    def strip_of(a, b):
        return 2 * a + (a + b) % 2

    def move(value, target):
        pairs = []
        for v in range(sections):
            for g in range(count):
                to = target(v // 2, v % 2, g // 2, g % 2)
                if to is not None:
                    pairs.append((v * count + g, (2 * to[0] + to[1]) * count + 2 * to[2] + to[3]))
        return lax.ppermute(value, AXES, pairs)

    def along_z(step):
        def target(a, c, k, b):
            return (a, c, k + step, b) if 0 <= k + step < count // 2 else None

        return target

    def along_x(step):
        def target(a, c, k, b):
            strip = strip_of(a, b) + step
            if not 0 <= strip < 4:
                return None
            return (strip // 2, c, k, (strip % 2 + strip // 2) % 2)

        return target

    partners = (
        lambda a, c, k, b: (a, c, k, 1 - b),
        lambda a, c, k, b: (1 - a, c, k, b),
        lambda a, c, k, b: (1 - a, c, k, 1 - b),
    )
    core_swap = lambda a, c, k, b: (a, 1 - c, k, b)

    def rows_for(block, a, b):
        return lax.dynamic_slice_in_dim(block, strip_of(a, b) * share, share, 1)

    def in_order(first_is_mine, mine, theirs):
        return jnp.concatenate(
            [jnp.where(first_is_mine, mine, theirs), jnp.where(first_is_mine, theirs, mine)], axis=0
        )

    kern = jnp.sum(jnp.where(jnp.arange(psf_table.shape[0])[:, None, None] == psf_index[0], psf_table, 0.0), axis=0)
    kern = kern / jnp.sum(kern, axis=-1, keepdims=True)
    other = move(kern, partners[1])
    kerns = (jnp.where(a == 0, kern, other), jnp.where(a == 0, other, kern))
    setups = []
    for kern in kerns:
        flipped = kern[:, ::-1]
        mat_y = banded(kern[2], width_y, width_y, pad)
        setups.append((
            kern[0], x_matrix(kern[1], share, pad), mat_y.T, x_matrix(flipped[1], share, pad), mat_y
        ))

    theirs = rows_for(start, a, 1 - b)
    part = move(lax.dynamic_slice_in_dim(theirs, c * half, half, 0), partners[0])
    theirs = in_order(c == 0, part, move(part, core_swap))
    estimate = in_order(b == 0, rows_for(start, a, b), theirs)

    mine = rows_for(slab, a, b)
    from_y = move(rows_for(slab, a, 1 - b), partners[0])
    from_x = move(rows_for(slab, 1 - a, b), partners[1])
    from_xy = move(rows_for(slab, 1 - a, 1 - b), partners[2])
    data = tuple(
        in_order(b == 0, jnp.where(a == high, mine, from_x), jnp.where(a == high, from_y, from_xy))
        for high in range(2)
    )

    for step in range(ITERS):
        low = move(estimate[:, share - pad:], along_x(1))
        high = move(estimate[:, :pad], along_x(-1))
        wide = jnp.concatenate([low, estimate, high], axis=1)
        low = move(wide[2 * planes - pad:], along_z(1))
        high = move(wide[:pad], along_z(-1))
        wide = jnp.concatenate([low, wide, high], axis=0)
        smeared = []
        for which in range(2):
            kz, ax, my = setups[which][:3]
            ratio = blur_forward(kz, wide, data[which], ax, my)
            low = move(ratio[2 * planes - pad:], along_z(1))
            high = move(ratio[:pad], along_z(-1))
            smeared.append((low, ratio, high))
        edges = []
        for which in range(2):
            u = smear(setups[which][0], *smeared[which])
            low = move(u[:, share - pad:], along_x(1))
            high = move(u[:, :pad], along_x(-1))
            edges.append((low, u, high))
        product = None
        for which in range(2):
            ax, my = setups[which][3:]
            product = blur_back(*edges[which], ax, my, product)
        total = product * move(product, core_swap)
        estimate = estimate * jnp.sqrt(jnp.sqrt(total))

    def piece(b):
        return lax.dynamic_slice_in_dim(estimate, planes * b + half * c, half, 0)

    got = (
        piece(b),
        move(piece(1 - b), partners[0]),
        move(piece(b), partners[1]),
        move(piece(1 - b), partners[2]),
    )
    strips = []
    for strip in range(4):
        at_a = strip // 2
        at_b = (strip % 2 + at_a) % 2
        same_a, same_b = a == at_a, b == at_b
        strips.append(jnp.where(
            same_a, jnp.where(same_b, got[0], got[1]), jnp.where(same_b, got[2], got[3])
        ))
    whole = jnp.concatenate(strips, axis=1)
    return in_order(c == 0, whole, move(whole, core_swap))


def solution(mesh):
    return jax.shard_map(
        functools.partial(on_device, mesh.shape["view"], mesh.shape["gz"]),
        mesh=mesh,
        in_specs=(P("view", "gz", None, None), P("gz", None, None), P(), P("view")),
        out_specs=P("gz", None, None),
        check_vma=False,
    )
```
